32 devices in a mesh: rows: 4 (over x, core), seq: 8 (over z, y).
Axes of the slice: x: 2, y: 2, z: 4, core: 2. Of those that a mesh axis runs over, the one named last changes fastest.
Arguments:
- layer_in: bfloat16 [32, 1024, 768], P('rows', 'seq'), may hold values from -6 to 6
- cotangent: bfloat16 [32, 1024, 768], P('rows', 'seq'), may hold values from -6 to 6
- seg_lengths: int32 [32, 4], P('rows'), may hold values from 1 to 384, as said below
- query_weight: bfloat16 [768, 768], P(('rows', 'seq')), may hold values from -0.21875 to 0.21875
- query_bias: bfloat16 [768], P(('rows', 'seq')), may hold values from -3 to 3
- key_weight: bfloat16 [768, 768], P(('rows', 'seq')), may hold values from -0.21875 to 0.21875
- value_weight: bfloat16 [768, 768], P(('rows', 'seq')), may hold values from -0.21875 to 0.21875
- value_bias: bfloat16 [768], P(('rows', 'seq')), may hold values from -3 to 3
- out_weight: bfloat16 [768, 768], P(('rows', 'seq')), may hold values from -0.875 to 0.875
- out_bias: bfloat16 [768], P(('rows', 'seq')), may hold values from -2 to 2
- attn_gain: bfloat16 [768], P(('rows', 'seq')), may hold values from 0.5 to 1.5
- attn_shift: bfloat16 [768], P(('rows', 'seq')), may hold values from -2 to 2
- inner_weight: bfloat16 [768, 3072], P(('rows', 'seq')), may hold values from -0.21875 to 0.21875
- inner_bias: bfloat16 [3072], P(('rows', 'seq')), may hold values from -3 to 3
- outer_weight: bfloat16 [3072, 768], P(('rows', 'seq')), may hold values from -0.21875 to 0.21875
- outer_bias: bfloat16 [768], P(('rows', 'seq')), may hold values from -2 to 2
- final_gain: bfloat16 [768], P(('rows', 'seq')), may hold values from 0.5 to 1.5
- final_shift: bfloat16 [768], P(('rows', 'seq')), may hold values from -2 to 2
Outputs:
- layer_out: bfloat16 [32, 1024, 768], P('rows', 'seq')
- grad_in: float32 [32, 1024, 768], P('rows', 'seq')
- grad_query_weight: float32 [768, 768], P(('rows', 'seq'))
- grad_query_bias: float32 [768], P(('rows', 'seq'))
- grad_key_weight: float32 [768, 768], P(('rows', 'seq'))
- grad_value_weight: float32 [768, 768], P(('rows', 'seq'))
- grad_value_bias: float32 [768], P(('rows', 'seq'))
- grad_out_weight: float32 [768, 768], P(('rows', 'seq'))
- grad_out_bias: float32 [768], P(('rows', 'seq'))
- grad_attn_gain: float32 [768], P(('rows', 'seq'))
- grad_attn_shift: float32 [768], P(('rows', 'seq'))
- grad_inner_weight: float32 [768, 3072], P(('rows', 'seq'))
- grad_inner_bias: float32 [3072], P(('rows', 'seq'))
- grad_outer_weight: float32 [3072, 768], P(('rows', 'seq'))
- grad_outer_bias: float32 [768], P(('rows', 'seq'))
- grad_final_gain: float32 [768], P(('rows', 'seq'))
- grad_final_shift: float32 [768], P(('rows', 'seq'))
The draws below stay inside these ranges and needn't reach their ends.
Inputs may be any that keep to these rules, and one draw needn't show every extreme that they name: `seg_lengths`: the lengths of each row sum to 960, and the positions past their sum are padding; the last segment of each row has exactly 384 tokens.
All inputs are finite; a program needn't handle non-finite values.
Results may differ from the reference program's by a relative error of at most 0.015.
Values may be sent and summed in bfloat16 or wider, within the bound.
A program may use at most 256 MiB of HBM per device.

```python
import jax
import jax.numpy as jnp
from jax import lax

D = 768
HEADS = 12
HEAD_DIM = 64
FF = 3072
BLK = 128
MOST = 384
ROW_LEN = 1024
ROWS = 32
NSEG = 4


def draw_seg_lengths(key, part):
    total = ROW_LEN - BLK // 2
    remain = total - MOST
    parts_count = NSEG - 1
    base = remain // parts_count
    extra = remain - base * parts_count
    spread = min(base - 1, MOST - base - 1) // 2
    columns = jnp.arange(parts_count, dtype=jnp.int32)
    base_row = base + (columns < extra).astype(jnp.int32)
    offsets = jax.random.randint(jax.random.fold_in(key, 11), (ROWS, parts_count - 1), -spread, spread + 1)
    zero_col = jnp.zeros((ROWS, 1), jnp.int32)
    upper = jnp.concatenate([offsets, zero_col], axis=1)
    lower = jnp.concatenate([zero_col, offsets], axis=1)
    front = base_row[None, :] + upper - lower
    last_col = jnp.full((ROWS, 1), MOST, jnp.int32)
    return jnp.concatenate([front, last_col], axis=1).astype(jnp.int32)


def block_scale(key, dims, shards, smallest, largest):
    def one(position, parts):
        draws = jax.random.uniform(jax.random.fold_in(jax.random.fold_in(key, 6), position), (parts,), jnp.float32, smallest / len(shards), largest / len(shards))
        return jnp.repeat(jnp.exp(draws), dims[position] // parts).reshape((-1,) + (1,) * (len(dims) - position - 1))

    level = one(*shards[0])
    for cut in shards[1:]:
        level = level * one(*cut)
    return level


def gaussian(rng, shape, scale, bound, shards=(), held_as=jnp.bfloat16):
    array = jax.random.normal(rng, shape, jnp.float32) * scale
    if len(shards) > 0:
        array = block_scale(rng, shape, shards, -0.22, 0.18) * array
    return jnp.clip(array, min=-bound, max=bound).astype(held_as)


def setup_inputs(seed: int = 0) -> dict:
    key_list = jax.random.split(jax.random.key(seed), 19)
    layer_in = gaussian(key_list[0], (ROWS, ROW_LEN, D), 1.0, 6.0, ((0, 4), (1, 8)))
    cotangent = gaussian(key_list[1], (ROWS, ROW_LEN, D), 1.0, 6.0, ((0, 4), (1, 8)))
    seg_lengths = draw_seg_lengths(jax.random.fold_in(key_list[18], 71), 0)
    query_weight = gaussian(key_list[3], (D, D), D ** -0.5, 0.21875, ((0, 32),))
    query_bias = gaussian(key_list[4], (D,), 0.5, 3.0, ((0, 32),))
    key_weight = gaussian(key_list[5], (D, D), D ** -0.5, 0.21875, ((0, 32),))
    value_weight = gaussian(key_list[6], (D, D), D ** -0.5, 0.21875, ((0, 32),))
    value_bias = gaussian(key_list[7], (D,), 0.5, 3.0, ((0, 32),))
    out_weight = gaussian(key_list[8], (D, D), (D // 16) ** -0.5, 0.875, ((0, 32),))
    out_bias = gaussian(key_list[9], (D,), 0.3, 2.0, ((0, 32),))
    attn_gain = jnp.clip(1.0 + 0.1 * jax.random.normal(key_list[10], (D,), jnp.float32), 0.5, 1.5).astype(jnp.bfloat16)
    attn_shift = gaussian(key_list[11], (D,), 0.3, 2.0, ((0, 32),))
    inner_weight = gaussian(key_list[12], (D, FF), D ** -0.5, 0.21875, ((0, 32),))
    inner_bias = gaussian(key_list[13], (FF,), 0.5, 3.0, ((0, 32),))
    outer_weight = gaussian(key_list[14], (FF, D), (FF // 4) ** -0.5, 0.21875, ((0, 32),))
    outer_bias = gaussian(key_list[15], (D,), 0.3, 2.0, ((0, 32),))
    final_gain = jnp.clip(1.0 + 0.1 * jax.random.normal(key_list[16], (D,), jnp.float32), 0.5, 1.5).astype(jnp.bfloat16)
    final_shift = gaussian(key_list[17], (D,), 0.3, 2.0, ((0, 32),))
    return {"layer_in": layer_in, "cotangent": cotangent, "seg_lengths": seg_lengths, "query_weight": query_weight, "query_bias": query_bias, "key_weight": key_weight, "value_weight": value_weight, "value_bias": value_bias, "out_weight": out_weight, "out_bias": out_bias, "attn_gain": attn_gain, "attn_shift": attn_shift, "inner_weight": inner_weight, "inner_bias": inner_bias, "outer_weight": outer_weight, "outer_bias": outer_bias, "final_gain": final_gain, "final_shift": final_shift}


@jax.custom_vjp
def low(v):
    return lax.optimization_barrier(v.astype(jnp.bfloat16)).astype(jnp.float32)

@jax.custom_vjp
def low_back(v):
    return v

def low_keep(v):
    return (low(v), None)

def low_pass(kept, grad):
    return (grad,)

def back_keep(v):
    return (v, None)

def back_low(kept, grad):
    return (low(grad),)
low.defvjp(low_keep, low_pass)
low_back.defvjp(back_keep, back_low)
epsilon = 1e-12
masked_score = -1e+30

def product(left, right):
    return jnp.dot(left, right, precision=lax.Precision.HIGHEST, preferred_element_type=jnp.float32)

def normalize(values, gain_vec, shift_vec):
    row_mean = lax.optimization_barrier(jnp.mean(values, axis=-1, keepdims=True))
    centred = values - row_mean
    variance = lax.optimization_barrier(jnp.mean(centred * centred, axis=-1, keepdims=True))
    return centred * lax.rsqrt(variance + epsilon) * gain_vec + shift_vec

def segment_ids(lengths, positions, row_len):
    seg_ends = jnp.cumsum(lengths, axis=1)
    seg_count = lax.optimization_barrier(jnp.sum((positions[None, None, :] >= seg_ends[:, :, None]).astype(jnp.int32), axis=1))
    real_token = positions[None, :] < seg_ends[:, -1:]
    return jnp.where(real_token, seg_count, row_len + positions[None, :]).astype(jnp.int32)

def attend_row(pieces):
    query_rows, key_rows, value_rows, seg_id = pieces
    scores = jnp.einsum('qhd,khd->hqk', query_rows, key_rows, precision=lax.Precision.HIGHEST) * HEAD_DIM ** (-0.5)
    scores = low_back(scores)
    same_segment = seg_id[:, None] == seg_id[None, :]
    scores = jnp.where(same_segment[None], scores, masked_score)
    row_max = lax.optimization_barrier(jnp.max(scores, axis=-1, keepdims=True))
    weights = jnp.exp(scores - row_max)
    probs = low(weights / lax.optimization_barrier(jnp.sum(weights, axis=-1, keepdims=True)))
    return jnp.einsum('hqk,khd->qhd', probs, value_rows, precision=lax.Precision.HIGHEST)

def forward(layer_float, seg_id, query_weight, query_bias, key_weight, value_weight, value_bias, out_weight, out_bias, attn_gain, attn_shift, inner_weight, inner_bias, outer_weight, outer_bias, final_gain, final_shift):
    row_count, row_len, features = layer_float.shape
    flat = layer_float.reshape(row_count * row_len, features)
    flat_low = low(flat)
    query_all = low(low_back(product(flat_low, query_weight) + query_bias))
    key_all = low(low_back(product(flat_low, key_weight)))
    value_all = low(low_back(product(flat_low, value_weight) + value_bias))
    head_shape = (row_count, row_len, HEADS, HEAD_DIM)
    context = lax.map(jax.checkpoint(attend_row), (query_all.reshape(head_shape), key_all.reshape(head_shape), value_all.reshape(head_shape), seg_id))
    context = low(low_back(context.reshape(row_count * row_len, features)))
    attended = low_back(product(context, out_weight) + out_bias)
    hidden = normalize(flat + attended, attn_gain, attn_shift)
    inner_pre = low_back(product(low(hidden), inner_weight) + inner_bias)
    active = low(jax.nn.gelu(inner_pre, approximate=False))
    outer_out = low_back(product(active, outer_weight) + outer_bias)
    result = normalize(hidden + outer_out, final_gain, final_shift)
    return result.reshape(row_count, row_len, features)

def reference(layer_in, cotangent, seg_lengths, query_weight, query_bias, key_weight, value_weight, value_bias, out_weight, out_bias, attn_gain, attn_shift, inner_weight, inner_bias, outer_weight, outer_bias, final_gain, final_shift):
    row_len = layer_in.shape[1]
    positions = jnp.arange(row_len, dtype=jnp.int32)
    seg_id = segment_ids(seg_lengths, positions, row_len)
    real_token = (positions[None, :] < lax.optimization_barrier(jnp.sum(seg_lengths, axis=1))[:, None]).astype(jnp.float32)

    def layer_fn(layer_float, p_qw, p_qb, p_kw, p_vw, p_vb, p_ow, p_ob, p_ag, p_as, p_iw, p_ib, p_tw, p_tb, p_fg, p_fs):
        return forward(layer_float, seg_id, p_qw, p_qb, p_kw, p_vw, p_vb, p_ow, p_ob, p_ag, p_as, p_iw, p_ib, p_tw, p_tb, p_fg, p_fs)
    result, pullback = jax.vjp(layer_fn, layer_in.astype(jnp.float32), query_weight.astype(jnp.float32), query_bias.astype(jnp.float32), key_weight.astype(jnp.float32), value_weight.astype(jnp.float32), value_bias.astype(jnp.float32), out_weight.astype(jnp.float32), out_bias.astype(jnp.float32), attn_gain.astype(jnp.float32), attn_shift.astype(jnp.float32), inner_weight.astype(jnp.float32), inner_bias.astype(jnp.float32), outer_weight.astype(jnp.float32), outer_bias.astype(jnp.float32), final_gain.astype(jnp.float32), final_shift.astype(jnp.float32))
    upstream = cotangent.astype(jnp.float32) * real_token[:, :, None]
    g_in, g_qw, g_qb, g_kw, g_vw, g_vb, g_ow, g_ob, g_ag, g_as, g_iw, g_ib, g_tw, g_tb, g_fg, g_fs = pullback(upstream)
    return (result.astype(jnp.bfloat16), g_in, g_qw, g_qb, g_kw, g_vw, g_vb, g_ow, g_ob, g_ag, g_as, g_iw, g_ib, g_tw, g_tb, g_fg, g_fs)
```

```python
from functools import partial

import jax
import jax.numpy as jnp
from jax import lax
from jax.experimental import pallas as pl
from jax.experimental.pallas import tpu as pltpu
from jax.sharding import PartitionSpec as P

HEADS = 12
HEAD_DIM = 64
REACH = 3


epsilon = 1e-12
masked_score = -1e30


def passed_along(block, axis, distance):
    devices = range(lax.axis_size(axis))
    route = [(i - distance, i) for i in devices if i - distance in devices]
    return lax.ppermute(block, axis, route)


def segment_ids(lengths, positions, row_len):
    seg_ends = jnp.cumsum(lengths, axis=1)
    seg_count = jnp.sum(
        (positions[None, None, :] >= seg_ends[:, :, None]).astype(jnp.int32), axis=1
    )
    real_token = positions[None, :] < seg_ends[:, -1:]
    inside = (positions >= 0) & (positions < row_len)
    seg_id = jnp.where(real_token, seg_count, row_len + positions[None, :])
    return jnp.where(inside[None, :], seg_id, -1)


def norm_parts(values):
    row_mean = jnp.mean(values, axis=-1, keepdims=True)
    centred = values - row_mean
    inv_std = lax.rsqrt(jnp.mean(centred * centred, axis=-1, keepdims=True) + epsilon)
    return (centred * inv_std, inv_std)


def norm_back(upstream, normed, inv_std, gain_vec):
    scaled = upstream * gain_vec
    return inv_std * (
        scaled
        - jnp.mean(scaled, axis=-1, keepdims=True)
        - normed * jnp.mean(scaled * normed, axis=-1, keepdims=True)
    )


def split_window(window, features):
    key_rows = window[:, :features].reshape(window.shape[0], HEADS, HEAD_DIM)
    value_rows = window[:, features:].reshape(window.shape[0], HEADS, HEAD_DIM)
    return (key_rows, value_rows)


def row_scores(query_rows, key_rows, same_segment, score_scale):
    scores = (
        jnp.einsum("qhd,khd->hqk", query_rows, key_rows, preferred_element_type=jnp.float32)
        * score_scale
    )
    return jnp.where(same_segment[None], scores, masked_score)


def attend_row(pieces, score_scale):
    query_rows, window, same_segment = pieces
    key_rows, value_rows = split_window(window, query_rows.shape[1] * query_rows.shape[2])
    scores = row_scores(query_rows, key_rows, same_segment, score_scale)
    row_max = jnp.max(scores, axis=-1, keepdims=True)
    weights = jnp.exp(scores - row_max)
    row_total = jnp.sum(weights, axis=-1, keepdims=True)
    weights_b = (weights / row_total).astype(jnp.bfloat16)
    context = jnp.einsum("hqk,khd->qhd", weights_b, value_rows, preferred_element_type=jnp.float32)
    return (context.astype(jnp.bfloat16), (row_max + jnp.log(row_total))[..., 0])


def attend_back(pieces, score_scale):
    query_rows, window, same_segment, logsum, grad_context = pieces
    features = query_rows.shape[1] * query_rows.shape[2]
    key_rows, value_rows = split_window(window, features)
    scores = row_scores(query_rows, key_rows, same_segment, score_scale)
    probs = jnp.exp(scores - logsum[..., None])
    grad_probs = jnp.einsum(
        "qhd,khd->hqk", grad_context, value_rows, preferred_element_type=jnp.float32
    )
    grad_scores = (
        probs * (grad_probs - jnp.sum(grad_probs * probs, axis=-1, keepdims=True))
    ).astype(jnp.bfloat16)
    grad_query = (
        jnp.einsum("hqk,khd->qhd", grad_scores, key_rows, preferred_element_type=jnp.float32)
        * score_scale
    )
    grad_key = (
        jnp.einsum("hqk,qhd->khd", grad_scores, query_rows, preferred_element_type=jnp.float32)
        * score_scale
    )
    grad_value = jnp.einsum(
        "hqk,qhd->khd", probs.astype(jnp.bfloat16), grad_context, preferred_element_type=jnp.float32
    )
    width_keys = window.shape[0]
    return (
        grad_query,
        jnp.concatenate(
            [grad_key.reshape(width_keys, features), grad_value.reshape(width_keys, features)],
            axis=1,
        ),
    )


def near_distances():
    return list(range(REACH, 0, -1)) + list(range(-1, -REACH - 1, -1))


def near_window(kv_local):
    lower_side = []
    upper_side = []
    for distance in near_distances():
        arrived = passed_along(kv_local, "seq", distance)
        if distance > 0:
            lower_side.append(arrived)
        else:
            upper_side.append(arrived)
    return jnp.concatenate(lower_side + [kv_local] + upper_side, axis=1)


def near_back(grad_window, block_len):
    own_grad = grad_window[:, REACH * block_len : (REACH + 1) * block_len]
    for position in range(2 * REACH + 1):
        offset = position - REACH
        if offset != 0:
            grad_piece = grad_window[:, position * block_len : (position + 1) * block_len]
            own_grad = own_grad + passed_along(
                grad_piece.astype(jnp.bfloat16), "seq", offset
            ).astype(grad_piece.dtype)
    return own_grad


def body(
    layer_in,
    cotangent,
    seg_lengths,
    query_weight,
    query_bias,
    key_weight,
    value_weight,
    value_bias,
    out_weight,
    out_bias,
    attn_gain,
    attn_shift,
    inner_weight,
    inner_bias,
    outer_weight,
    outer_bias,
    final_gain,
    final_shift,
):
    shards = (
        query_weight,
        query_bias,
        key_weight,
        value_weight,
        value_bias,
        out_weight,
        out_bias,
        attn_gain,
        attn_shift,
        inner_weight,
        inner_bias,
        outer_weight,
        outer_bias,
        final_gain,
        final_shift,
    )
    gathered = (
        lax.all_gather(shards[0], ("rows", "seq"), axis=0, tiled=True),
        lax.all_gather(shards[1], ("rows", "seq"), axis=0, tiled=True),
        lax.all_gather(shards[2], ("rows", "seq"), axis=0, tiled=True),
        lax.all_gather(shards[3], ("rows", "seq"), axis=0, tiled=True),
        lax.all_gather(shards[4], ("rows", "seq"), axis=0, tiled=True),
        lax.all_gather(shards[5], ("rows", "seq"), axis=0, tiled=True),
        lax.all_gather(shards[6], ("rows", "seq"), axis=0, tiled=True),
        lax.all_gather(shards[7], ("rows", "seq"), axis=0, tiled=True),
        lax.all_gather(shards[8], ("rows", "seq"), axis=0, tiled=True),
        lax.all_gather(shards[9], ("rows", "seq"), axis=0, tiled=True),
        lax.all_gather(shards[10], ("rows", "seq"), axis=0, tiled=True),
        lax.all_gather(shards[11], ("rows", "seq"), axis=0, tiled=True),
        lax.all_gather(shards[12], ("rows", "seq"), axis=0, tiled=True),
        lax.all_gather(shards[13], ("rows", "seq"), axis=0, tiled=True),
        lax.all_gather(shards[14], ("rows", "seq"), axis=0, tiled=True),
    )
    (
        query_mat,
        query_vec,
        key_mat,
        value_mat,
        value_vec,
        out_mat,
        out_vec,
        attn_gain_f,
        attn_shift_f,
        inner_mat,
        inner_vec,
        outer_mat,
        outer_vec,
        final_gain_f,
        final_shift_f,
    ) = gathered
    row_count, block_len, features = layer_in.shape
    tokens = row_count * block_len
    score_scale = HEAD_DIM ** (-0.5)
    inputs = layer_in.reshape(tokens, features)
    query_flat = jnp.dot(inputs, query_mat, preferred_element_type=jnp.float32) + query_vec.astype(
        jnp.float32
    )
    query_b = query_flat.astype(jnp.bfloat16).reshape(row_count, block_len, HEADS, HEAD_DIM)
    kv_mat = jnp.concatenate([key_mat, value_mat], axis=1)
    kv_bias = jnp.concatenate([jnp.zeros_like(value_vec), value_vec]).astype(jnp.float32)
    kv_local = (
        (jnp.dot(inputs, kv_mat, preferred_element_type=jnp.float32) + kv_bias)
        .astype(jnp.bfloat16)
        .reshape(row_count, block_len, 2 * features)
    )
    seq_index = lax.axis_index("seq")
    row_len = block_len * lax.axis_size("seq")
    local_pos = seq_index * block_len + jnp.arange(block_len, dtype=jnp.int32)
    window_pos = (seq_index - REACH) * block_len + jnp.arange(
        (2 * REACH + 1) * block_len, dtype=jnp.int32
    )
    query_ids = segment_ids(seg_lengths, local_pos, row_len)
    key_ids = segment_ids(seg_lengths, window_pos, row_len)
    same_segment = query_ids[:, :, None] == key_ids[:, None, :]
    window = near_window(kv_local)
    context, logsum = lax.map(
        partial(attend_row, score_scale=score_scale), (query_b, window, same_segment)
    )
    context_flat = context.reshape(tokens, features)
    attended = jnp.dot(context_flat, out_mat, preferred_element_type=jnp.float32) + out_vec.astype(
        jnp.float32
    )
    first_sum = inputs.astype(jnp.float32) + attended
    normed_one, inv_std_one = norm_parts(first_sum)
    hidden = normed_one * attn_gain_f.astype(jnp.float32) + attn_shift_f.astype(jnp.float32)
    hidden_b = hidden.astype(jnp.bfloat16)
    inner_pre = jnp.dot(hidden_b, inner_mat, preferred_element_type=jnp.float32) + inner_vec.astype(
        jnp.float32
    )
    active, gelu_back = jax.vjp(partial(jax.nn.gelu, approximate=False), inner_pre)
    active_b = active.astype(jnp.bfloat16)
    outer_out = jnp.dot(active_b, outer_mat, preferred_element_type=jnp.float32) + outer_vec.astype(
        jnp.float32
    )
    normed_two, inv_std_two = norm_parts(hidden + outer_out)
    layer_out = (
        normed_two * final_gain_f.astype(jnp.float32) + final_shift_f.astype(jnp.float32)
    ).astype(jnp.bfloat16)
    real_token = (local_pos[None, :] < jnp.sum(seg_lengths, axis=1)[:, None]).astype(jnp.float32)
    upstream = (cotangent.astype(jnp.float32) * real_token[:, :, None]).reshape(tokens, features)
    grad_final_gain = jnp.sum(upstream * normed_two, axis=0)
    grad_final_shift = jnp.sum(upstream, axis=0)
    grad_second = norm_back(upstream, normed_two, inv_std_two, final_gain_f.astype(jnp.float32))
    grad_outer = grad_second.astype(jnp.bfloat16)
    grad_outer_bias = jnp.sum(grad_outer.astype(jnp.float32), axis=0)
    grad_outer_weight = jnp.einsum(
        "tf,td->fd", active_b, grad_outer, preferred_element_type=jnp.float32
    )
    grad_active = jnp.einsum("td,fd->tf", grad_outer, outer_mat, preferred_element_type=jnp.float32)
    grad_inner = gelu_back(grad_active)[0].astype(jnp.bfloat16)
    grad_inner_bias = jnp.sum(grad_inner.astype(jnp.float32), axis=0)
    grad_inner_weight = jnp.einsum(
        "td,tf->df", hidden_b, grad_inner, preferred_element_type=jnp.float32
    )
    grad_hidden = grad_second + jnp.einsum(
        "tf,df->td", grad_inner, inner_mat, preferred_element_type=jnp.float32
    )
    grad_attn_gain = jnp.sum(grad_hidden * normed_one, axis=0)
    grad_attn_shift = jnp.sum(grad_hidden, axis=0)
    grad_first = norm_back(grad_hidden, normed_one, inv_std_one, attn_gain_f.astype(jnp.float32))
    grad_attended = grad_first.astype(jnp.bfloat16)
    grad_out_bias = jnp.sum(grad_attended.astype(jnp.float32), axis=0)
    grad_out_weight = jnp.einsum(
        "td,te->de", context_flat, grad_attended, preferred_element_type=jnp.float32
    )
    grad_context = jnp.einsum(
        "te,de->td", grad_attended, out_mat, preferred_element_type=jnp.float32
    ).astype(jnp.bfloat16)
    grad_context = grad_context.reshape(row_count, block_len, HEADS, HEAD_DIM)
    grad_query, grad_window = lax.map(
        partial(attend_back, score_scale=score_scale),
        (query_b, window, same_segment, logsum, grad_context),
    )
    grad_kv = near_back(grad_window, block_len)
    grad_query_b = grad_query.reshape(tokens, features).astype(jnp.bfloat16)
    grad_kv_b = grad_kv.reshape(tokens, 2 * features).astype(jnp.bfloat16)
    grad_query_weight = jnp.einsum(
        "td,te->de", inputs, grad_query_b, preferred_element_type=jnp.float32
    )
    grad_query_bias = jnp.sum(grad_query_b.astype(jnp.float32), axis=0)
    grad_kv_weight = jnp.einsum("td,te->de", inputs, grad_kv_b, preferred_element_type=jnp.float32)
    grad_value_bias = jnp.sum(grad_kv_b[:, features:].astype(jnp.float32), axis=0)
    grad_in = grad_first + jnp.einsum(
        "te,de->td", grad_query_b, query_mat, preferred_element_type=jnp.float32
    )
    grad_in = grad_in + jnp.einsum(
        "te,de->td", grad_kv_b, kv_mat, preferred_element_type=jnp.float32
    )
    partial_grads = (
        grad_query_weight,
        grad_query_bias,
        grad_kv_weight[:, :features],
        grad_kv_weight[:, features:],
        grad_value_bias,
        grad_out_weight,
        grad_out_bias,
        grad_attn_gain,
        grad_attn_shift,
        grad_inner_weight,
        grad_inner_bias,
        grad_outer_weight,
        grad_outer_bias,
        grad_final_gain,
        grad_final_shift,
    )
    owned = (
        lax.psum_scatter(partial_grads[0], ("rows", "seq"), scatter_dimension=0, tiled=True),
        lax.psum_scatter(partial_grads[1], ("rows", "seq"), scatter_dimension=0, tiled=True),
        lax.psum_scatter(partial_grads[2], ("rows", "seq"), scatter_dimension=0, tiled=True),
        lax.psum_scatter(partial_grads[3], ("rows", "seq"), scatter_dimension=0, tiled=True),
        lax.psum_scatter(partial_grads[4], ("rows", "seq"), scatter_dimension=0, tiled=True),
        lax.psum_scatter(partial_grads[5], ("rows", "seq"), scatter_dimension=0, tiled=True),
        lax.psum_scatter(partial_grads[6], ("rows", "seq"), scatter_dimension=0, tiled=True),
        lax.psum_scatter(partial_grads[7], ("rows", "seq"), scatter_dimension=0, tiled=True),
        lax.psum_scatter(partial_grads[8], ("rows", "seq"), scatter_dimension=0, tiled=True),
        lax.psum_scatter(partial_grads[9], ("rows", "seq"), scatter_dimension=0, tiled=True),
        lax.psum_scatter(partial_grads[10], ("rows", "seq"), scatter_dimension=0, tiled=True),
        lax.psum_scatter(partial_grads[11], ("rows", "seq"), scatter_dimension=0, tiled=True),
        lax.psum_scatter(partial_grads[12], ("rows", "seq"), scatter_dimension=0, tiled=True),
        lax.psum_scatter(partial_grads[13], ("rows", "seq"), scatter_dimension=0, tiled=True),
        lax.psum_scatter(partial_grads[14], ("rows", "seq"), scatter_dimension=0, tiled=True),
    )
    g_qw, g_qb, g_kw, g_vw, g_vb, g_ow, g_ob, g_ag, g_as, g_iw, g_ib, g_tw, g_tb, g_fg, g_fs = owned
    return (
        layer_out.reshape(row_count, block_len, features),
        grad_in.reshape(row_count, block_len, features),
        g_qw,
        g_qb,
        g_kw,
        g_vw,
        g_vb,
        g_ow,
        g_ob,
        g_ag,
        g_as,
        g_iw,
        g_ib,
        g_tw,
        g_tb,
        g_fg,
        g_fs,
    )


MESH = pl.DeviceIdType.MESH


def place():
    r = lax.axis_index("rows")
    s = lax.axis_index("seq")
    return r // 2, r % 2, s // 2, s % 2, r, s


def greet(x, c, r, s, seq_size):
    barrier = pltpu.get_barrier_semaphore()
    for k in range(1, seq_size):
        pl.semaphore_signal(
            barrier, inc=1, device_id=(r, lax.rem(s + k, seq_size)), device_id_type=MESH
        )
    pl.semaphore_signal(barrier, inc=1, device_id=((1 - x) * 2 + c, s), device_id_type=MESH)
    pl.semaphore_signal(barrier, inc=1, device_id=(x * 2 + 1 - c, s), device_id_type=MESH)
    pl.semaphore_wait(barrier, seq_size + 1)


def remote(src, dst, send, recv, device):
    return pltpu.make_async_remote_copy(
        src_ref=src, dst_ref=dst, send_sem=send, recv_sem=recv, device_id=device, device_id_type=MESH
    )


def column_view(ref, lo, width):
    def view(x, c, z, y):
        return ref.at[x, c, z, y, :, pl.ds(lo, width)]

    return view


def gather_kernel(
    depth, seq_size, lanes, qkv_s, out_s, inner_s, outer_s, vec_s, x_in, cot_in,
    qkv_g, out_g, inner_g, outer_g, vec_g, x_row, cot_row,
    z_send, z_recv, p_send, p_recv, c_send, c_recv, e_send, e_recv, own_sem,
):
    x, c, z, y, r, s = place()
    xo, co, yo = 1 - x, 1 - c, 1 - y
    every = slice(None)
    greet(x, c, r, s, seq_size)
    pieces = []
    for src, dst, lo, width, order in (
        (qkv_s, qkv_g, 0, lanes[0] // 2, 0),
        (qkv_s, qkv_g, lanes[0] // 2, lanes[0] // 2, 1),
        (vec_s, vec_g, 0, 128, 0),
        (out_s, out_g, 0, lanes[1] // 2, 0),
        (out_s, out_g, lanes[1] // 2, lanes[1] // 2, 1),
        (inner_s, inner_g, 0, lanes[2], 0),
        (outer_s, outer_g, 0, lanes[1], 1),
    ):
        pieces.append((src.at[:, pl.ds(lo, width)], column_view(dst, lo, width), order))
    count = len(pieces)
    dev_x, dev_c, dev_y = (xo * 2 + c, s), (x * 2 + co, s), (r, z * 2 + yo)

    def z_copy(i, k):
        src, view, _ = pieces[i]
        return remote(
            src, view(x, c, z, y), z_send.at[i, k - 1], z_recv.at[i, k - 1],
            (r, lax.rem(z + k, depth) * 2 + y),
        )

    def z_arrive(i, k):
        src, view, _ = pieces[i]
        return remote(
            src, view(x, c, lax.rem(z + depth - k, depth), y), z_send.at[i, k - 1],
            z_recv.at[i, k - 1], (r, s),
        )

    def second(i, mine):
        view, order = pieces[i][1], pieces[i][2]
        there = (view(x, c, every, y if mine else yo), view(x if mine else xo, c, every, y))[order]
        return remote(there, there, p_send.at[i, 0], p_recv.at[i, 0], (dev_y, dev_x)[order])

    def third(i, mine):
        view, order = pieces[i][1], pieces[i][2]
        there = (view(x if mine else xo, c, every, every), view(every, c, every, y if mine else yo))[order]
        return remote(there, there, p_send.at[i, 1], p_recv.at[i, 1], (dev_x, dev_y)[order])

    def cross(i, step, mine):
        view, order = pieces[i][1], pieces[i][2]
        cc = c if mine else co
        there = (
            (view(x, cc, every, y), view(x, cc, every, yo), view(xo, cc, every, every)),
            (view(x, cc, every, y), view(xo, cc, every, y), view(every, cc, every, yo)),
        )[order][step]
        return remote(there, there, c_send.at[i, step], c_recv.at[i, step], dev_c)

    def own(i):
        src, view, _ = pieces[i]
        return pltpu.make_async_copy(src, view(x, c, z, y), own_sem.at[i])

    def row_copy(which, k, mine):
        src, dst = ((x_in, x_row), (cot_in, cot_row))[which]
        peer = lax.rem(s + k, seq_size)
        slot = s if mine else lax.rem(s + seq_size - k, seq_size)
        return remote(
            src.at[peer], dst.at[slot], e_send.at[which, k - 1], e_recv.at[which, k - 1], (r, peer)
        )

    def row_own(which):
        src, dst = ((x_in, x_row), (cot_in, cot_row))[which]
        return pltpu.make_async_copy(src.at[s], dst.at[s], own_sem.at[count + which])

    for i in range(2):
        for k in range(1, depth):
            z_copy(i, k).start()
    for k in range(1, seq_size):
        row_copy(0, k, True).start()
    for i in range(2, count):
        for k in range(1, depth):
            z_copy(i, k).start()
    for i in range(count):
        own(i).start()
    row_own(0).start()
    for k in range(1, seq_size):
        row_copy(1, k, True).start()
    row_own(1).start()
    for i in range(count):
        own(i).wait()
        for k in range(1, depth):
            z_arrive(i, k).wait_recv()
        second(i, True).start()
        cross(i, 0, True).start()
    for i in range(count):
        second(i, False).wait_recv()
        third(i, True).start()
        cross(i, 1, True).start()
    for i in range(count):
        third(i, False).wait_recv()
        cross(i, 2, True).start()
    for which in range(2):
        row_own(which).wait()
        for k in range(1, seq_size):
            row_copy(which, k, False).wait_recv()
            row_copy(which, k, True).wait_send()
    for i in range(count):
        for step in range(3):
            cross(i, step, False).wait_recv()
            cross(i, step, True).wait_send()
        for k in range(1, depth):
            z_copy(i, k).wait_send()
        second(i, True).wait_send()
        third(i, True).wait_send()


def gather_all(shards, layer_in, cotangent, depth, seq_size):
    qkv, out, inner, outer, vec = shards
    count = 7
    shapes = [jax.ShapeDtypeStruct((2, 2, depth, 2) + a.shape, a.dtype) for a in shards]
    rows = jax.ShapeDtypeStruct(layer_in.shape, layer_in.dtype)
    hbm = pl.BlockSpec(memory_space=pl.ANY)
    dma = pltpu.SemaphoreType.DMA
    lanes = (qkv.shape[1], out.shape[1], inner.shape[1])
    return pl.pallas_call(
        partial(gather_kernel, depth, seq_size, lanes),
        out_shape=tuple(shapes) + (rows, rows),
        in_specs=[hbm] * 7,
        out_specs=(hbm,) * 7,
        scratch_shapes=[
            dma((count, depth - 1)), dma((count, depth - 1)), dma((count, 2)), dma((count, 2)),
            dma((count, 3)), dma((count, 3)), dma((2, seq_size - 1)), dma((2, seq_size - 1)),
            dma((count + 2,)),
        ],
        compiler_params=pltpu.CompilerParams(collective_id=0, has_side_effects=True),
        name="gather_all",
    )(qkv, out, inner, outer, vec, layer_in, cotangent)


def reduce_kernel(
    depth, seq_size, lanes, qkv_p, out_p, inner_p, outer_p, vec_p, lo_in, gi_in,
    qkv_r, out_r, inner_r, outer_r, vec_r, lo_row, gi_row, *scratch,
):
    x, c, z, y, r, s = place()
    xo, co, yo = 1 - x, 1 - c, 1 - y
    every = slice(None)
    count = 7
    first, middle, last = scratch[:5], scratch[5:12], scratch[12:17]
    tail = scratch[17:22]
    c_send, c_recv, p_send, p_recv, z_send, z_recv, e_send, e_recv, own_sem = scratch[22:]
    greet(x, c, r, s, seq_size)
    dev_x, dev_c, dev_y = (xo * 2 + c, s), (x * 2 + co, s), (r, z * 2 + yo)
    pieces = []
    for a, (src, lo, width, order) in enumerate((
        (0, 0, lanes[0] // 2, 0),
        (0, lanes[0] // 2, lanes[0] // 2, 1),
        (1, 0, lanes[1] // 2, 0),
        (1, lanes[1] // 2, lanes[1] // 2, 1),
        (2, 0, lanes[2], 0),
        (3, 0, lanes[1], 1),
        (4, 0, 128, 0),
    )):
        pieces.append((src, pl.ds(lo, width), order))
    partials = (qkv_p, out_p, inner_p, outer_p, vec_p)
    results = (qkv_r, out_r, inner_r, outer_r, vec_r)

    def cross(i):
        a, cols, _ = pieces[i]
        return remote(
            partials[a].at[:, co, :, :, :, cols], first[a].at[:, :, :, :, cols],
            c_send.at[i], c_recv.at[i], dev_c,
        )

    def second(i):
        a, cols, order = pieces[i]
        held = first[a]
        src = (held.at[xo, :, :, :, cols], held.at[:, :, yo, :, cols])[order]
        return remote(src, middle[i], p_send.at[i, 0], p_recv.at[i, 0], (dev_x, dev_y)[order])

    def third(i):
        a, cols, order = pieces[i]
        held = first[a]
        src = (held.at[x, :, yo, :, cols], held.at[xo, :, y, :, cols])[order]
        return remote(src, last[a].at[:, :, cols], p_send.at[i, 1], p_recv.at[i, 1], (dev_y, dev_x)[order])

    def along(i, k):
        a, cols, _ = pieces[i]
        zt = lax.rem(z + k, depth)
        return remote(
            first[a].at[x, zt, y, :, cols], tail[a].at[k - 1, :, cols],
            z_send.at[i, k - 1], z_recv.at[i, k - 1], (r, zt * 2 + y),
        )

    def add(dst, a_val, b_val):
        return (a_val.astype(jnp.float32) + b_val.astype(jnp.float32)).astype(dst.dtype)

    def row_copy(which, k, mine):
        src, dst = ((lo_in, lo_row), (gi_in, gi_row))[which]
        peer = lax.rem(s + k, seq_size)
        slot = s if mine else lax.rem(s + seq_size - k, seq_size)
        return remote(
            src.at[peer], dst.at[slot], e_send.at[which, k - 1], e_recv.at[which, k - 1], (r, peer)
        )

    def row_own(which):
        src, dst = ((lo_in, lo_row), (gi_in, gi_row))[which]
        return pltpu.make_async_copy(src.at[s], dst.at[s], own_sem.at[which])

    sequence = (4, 5, 0, 1, 2, 3, 6)
    for i in sequence:
        cross(i).start()
    for which in range(2):
        row_own(which).start()
        for k in range(1, seq_size):
            row_copy(which, k, True).start()
    for i in sequence:
        a, cols, order = pieces[i]
        cross(i).wait_recv()

        @pl.loop(0, 4 * depth)
        def _(n, a=a, cols=cols):
            n0, n1, n2 = n // (2 * depth), (n // 2) % depth, n % 2
            first[a][n0, n1, n2, :, cols] = add(
                first[a], first[a][n0, n1, n2, :, cols], partials[a][n0, c, n1, n2, :, cols]
            )

        second(i).start()
    for i in sequence:
        a, cols, order = pieces[i]
        second(i).wait_recv()

        @pl.loop(0, 2 * depth)
        def _(n, i=i, a=a, cols=cols, order=order):
            n0, n1 = n // 2, n % 2
            if order == 0:
                at = (x, n0, n1, slice(None), cols)
                come = (n0, n1)
            else:
                at = (n1, n0, y, slice(None), cols)
                come = (n1, n0)
            first[a][at] = add(first[a], first[a][at], middle[i][come])

        third(i).start()
    for i in sequence:
        a, cols, order = pieces[i]
        third(i).wait_recv()

        @pl.loop(0, depth)
        def _(n, a=a, cols=cols):
            at = (x, n, y, slice(None), cols)
            first[a][at] = add(first[a], first[a][at], last[a][n, :, cols])

        for k in range(1, depth):
            along(i, k).start()
    for i in sequence:
        a, cols, order = pieces[i]
        total = first[a][x, z, y, :, cols].astype(jnp.float32)
        for k in range(1, depth):
            along(i, k).wait_recv()
            total = total + tail[a][k - 1, :, cols].astype(jnp.float32)
        results[a][:, cols] = total
    for which in range(2):
        row_own(which).wait()
        for k in range(1, seq_size):
            row_copy(which, k, False).wait_recv()
            row_copy(which, k, True).wait_send()
    for i in sequence:
        cross(i).wait_send()
        second(i).wait_send()
        third(i).wait_send()
        for k in range(1, depth):
            along(i, k).wait_send()


def reduce_all(partials, layer_out, grad_in, depth, seq_size):
    count = 7
    hbm = pl.BlockSpec(memory_space=pl.ANY)
    vmem = pl.BlockSpec(memory_space=pltpu.VMEM)
    dma = pltpu.SemaphoreType.DMA
    lanes = (partials[0].shape[-1], partials[1].shape[-1], partials[2].shape[-1])
    blocks = [(p.shape[-2:], p.dtype) for p in partials]
    scratch = [pltpu.VMEM((2, depth, 2) + b, t) for b, t in blocks]
    for a, width, order in (
        (0, lanes[0] // 2, 0), (0, lanes[0] // 2, 1), (1, lanes[1] // 2, 0), (1, lanes[1] // 2, 1),
        (2, lanes[2], 0), (3, lanes[1], 1), (4, 128, 0),
    ):
        lead = ((depth, 2), (2, depth))[order]
        scratch.append(pltpu.VMEM(lead + (blocks[a][0][0], width), blocks[a][1]))
    scratch += [pltpu.VMEM((depth,) + b, t) for b, t in blocks]
    scratch += [pltpu.VMEM((depth - 1,) + b, t) for b, t in blocks]
    return pl.pallas_call(
        partial(reduce_kernel, depth, seq_size, lanes),
        out_shape=tuple(jax.ShapeDtypeStruct(b, jnp.float32) for b, _ in blocks)
        + (jax.ShapeDtypeStruct(layer_out.shape, layer_out.dtype), jax.ShapeDtypeStruct(grad_in.shape, grad_in.dtype)),
        in_specs=[vmem] * 5 + [hbm] * 2,
        out_specs=(vmem,) * 5 + (hbm,) * 2,
        scratch_shapes=scratch + [
            dma((count,)), dma((count,)), dma((count, 2)), dma((count, 2)),
            dma((count, depth - 1)), dma((count, depth - 1)),
            dma((2, seq_size - 1)), dma((2, seq_size - 1)), dma((2,)),
        ],
        compiler_params=pltpu.CompilerParams(
            collective_id=1, has_side_effects=True, vmem_limit_bytes=60 * 1024 * 1024
        ),
        name="reduce_all",
    )(*partials, layer_out, grad_in)


FIRST_TILES = ((0, 128, 0, 512), (128, 128, 0, 576), (256, 128, 0, 576), (384, 128, 0, 576), (512, 64, 128, 448))
LAST_TILES = ((576, 128, 576, 384), (704, 128, 576, 384), (832, 128, 576, 384))
TILES = FIRST_TILES + LAST_TILES
REAL = 960


def both_heads(block):
    low = lax.broadcasted_iota(jnp.int32, block.shape, 1) < HEAD_DIM
    zero = jnp.zeros_like(block)
    return jnp.concatenate([jnp.where(low, block, zero), jnp.where(low, zero, block)], axis=0)


def pick_heads(wide, count):
    low = lax.broadcasted_iota(jnp.int32, (2 * HEAD_DIM, count), 0) < HEAD_DIM
    return jnp.where(low, wide[:, :count], wide[:, count:])


def tile_scores(q_both, keys, seg_col, seg_row, tile, masked):
    q0, qn, k0, kn = tile
    scores = lax.dot_general(
        keys, q_both, (((1,), (1,)), ((), ())), preferred_element_type=jnp.float32
    )
    if masked:
        queries = seg_row[:, q0 : q0 + qn]
        queries = jnp.concatenate([queries, queries], axis=1)
        scores = jnp.where(seg_col[k0 : k0 + kn, :] == queries, scores, masked_score)
    return scores


def attend_kernel(q_ref, k_ref, v_ref, seg_col, seg_row, ctx_ref, lse_ref):
    for n, tile in enumerate(TILES):
        q0, qn, k0, kn = tile
        q_both = both_heads(q_ref[q0 : q0 + qn, :] * jnp.bfloat16(HEAD_DIM**-0.5))
        scores = tile_scores(q_both, k_ref[k0 : k0 + kn, :], seg_col, seg_row, tile, n < 5)
        top = jnp.max(scores, axis=0, keepdims=True)
        weights = jnp.exp(scores - top)
        total = jnp.sum(weights, axis=0, keepdims=True)
        probs = (weights * (1.0 / total)).astype(jnp.bfloat16)
        lse_ref[0, n : n + 1, : 2 * qn] = top + jnp.log(total)
        wide = lax.dot_general(
            v_ref[k0 : k0 + kn, :], probs, (((0,), (0,)), ((), ())), preferred_element_type=jnp.float32
        )
        ctx_ref[q0 : q0 + qn, :] = pick_heads(wide, qn).T.astype(jnp.bfloat16)
    ctx_ref[REAL:, :] = v_ref[REAL:, :]


def attend(qkv, seg_col, seg_row):
    tokens, features = qkv.shape[0], qkv.shape[1] // 3
    pairs = features // 128

    def part(j):
        return pl.BlockSpec((tokens, 128), lambda p, j=j: (0, j * pairs + p))

    whole = lambda shape: pl.BlockSpec(shape, lambda p: (0,) * len(shape))
    return pl.pallas_call(
        attend_kernel,
        grid=(pairs,),
        out_shape=(
            jax.ShapeDtypeStruct((tokens, features), jnp.bfloat16),
            jax.ShapeDtypeStruct((pairs, 8, 256), jnp.float32),
        ),
        in_specs=[part(0), part(1), part(2), whole((tokens, 1)), whole((1, tokens))],
        out_specs=(
            pl.BlockSpec((tokens, 128), lambda p: (0, p)),
            pl.BlockSpec((1, 8, 256), lambda p: (p, 0, 0)),
        ),
        name="attend",
    )(qkv, qkv, qkv, seg_col, seg_row)


def attend_back_kernel(q_ref, k_ref, v_ref, g_ref, lse_ref, seg_col, seg_row, d_ref, dk_acc, dv_acc):
    features = d_ref.shape[1] // 3
    dk_acc[...] = jnp.zeros_like(dk_acc)
    dv_acc[...] = jnp.zeros_like(dv_acc)
    base = pl.program_id(0) * 128
    q_cols = pl.ds(pl.multiple_of(base, 128), 128)
    k_cols = pl.ds(pl.multiple_of(base + features, 128), 128)
    v_cols = pl.ds(pl.multiple_of(base + 2 * features, 128), 128)
    scale = HEAD_DIM**-0.5
    for n, tile in enumerate(TILES):
        q0, qn, k0, kn = tile
        keys, values = k_ref[k0 : k0 + kn, :], v_ref[k0 : k0 + kn, :]
        q_both = both_heads(q_ref[q0 : q0 + qn, :] * jnp.bfloat16(scale))
        g_both = both_heads(g_ref[q0 : q0 + qn, :])
        scores = tile_scores(q_both, keys, seg_col, seg_row, tile, n < 5)
        probs = jnp.exp(scores - lse_ref[0, n : n + 1, : 2 * qn])
        grad_probs = lax.dot_general(
            values, g_both, (((1,), (1,)), ((), ())), preferred_element_type=jnp.float32
        )
        dots = jnp.sum(probs * grad_probs, axis=0, keepdims=True)
        grad_scores = (probs * (grad_probs - dots)).astype(jnp.bfloat16)
        dv_acc[k0 : k0 + kn, :] += jnp.dot(
            probs.astype(jnp.bfloat16), g_both, preferred_element_type=jnp.float32
        )
        dk_acc[k0 : k0 + kn, :] += jnp.dot(grad_scores, q_both, preferred_element_type=jnp.float32)
        wide = lax.dot_general(
            keys, grad_scores, (((0,), (0,)), ((), ())), preferred_element_type=jnp.float32
        )
        d_ref[q0 : q0 + qn, q_cols] = (pick_heads(wide, qn).T * scale).astype(jnp.bfloat16)
    d_ref[:REAL, k_cols] = dk_acc[...].astype(jnp.bfloat16)
    d_ref[:REAL, v_cols] = dv_acc[...].astype(jnp.bfloat16)
    pad = g_ref[REAL:, :]
    d_ref[REAL:, q_cols] = jnp.zeros_like(pad)
    d_ref[REAL:, k_cols] = jnp.zeros_like(pad)
    d_ref[REAL:, v_cols] = pad


def attend_grad(qkv, grad_context, lse, seg_col, seg_row):
    tokens, features = grad_context.shape
    pairs = features // 128

    def part(j):
        return pl.BlockSpec((tokens, 128), lambda p, j=j: (0, j * pairs + p))

    whole = lambda shape: pl.BlockSpec(shape, lambda p: (0,) * len(shape))
    return pl.pallas_call(
        attend_back_kernel,
        grid=(pairs,),
        out_shape=jax.ShapeDtypeStruct((tokens, 3 * features), jnp.bfloat16),
        in_specs=[
            part(0), part(1), part(2), part(0), pl.BlockSpec((1, 8, 256), lambda p: (p, 0, 0)),
            whole((tokens, 1)), whole((1, tokens)),
        ],
        out_specs=whole((tokens, 3 * features)),
        scratch_shapes=[pltpu.VMEM((REAL, 128), jnp.float32), pltpu.VMEM((REAL, 128), jnp.float32)],
        name="attend_grad",
    )(qkv, qkv, qkv, grad_context, lse, seg_col, seg_row)


def gelu_parts(u):
    cdf = 0.5 * (1.0 + lax.erf(u * (2.0**-0.5)))
    density = jnp.exp(-0.5 * u * u) * ((2.0 * jnp.pi) ** -0.5)
    return u * cdf, cdf + u * density


def row_body(
    layer_in, cotangent, seg_lengths, query_weight, query_bias, key_weight, value_weight, value_bias,
    out_weight, out_bias, attn_gain, attn_shift, inner_weight, inner_bias, outer_weight, outer_bias,
    final_gain, final_shift,
):
    f32, bf16 = jnp.float32, jnp.bfloat16
    row_count, block_len, features = layer_in.shape
    seq_size = lax.axis_size("seq")
    depth = seq_size // 2
    devices = seq_size * lax.axis_size("rows")
    tokens = row_count * block_len
    hidden_units = inner_weight.shape[1]
    narrow = query_bias.shape[0]
    vectors = (
        query_bias, value_bias, out_bias, attn_gain, attn_shift, outer_bias, final_gain, final_shift, inner_bias,
    )
    packed = jnp.concatenate(vectors)
    packed = jnp.pad(packed, (0, 1024 - packed.shape[0])).reshape(8, 128)
    shards = (
        jnp.concatenate([query_weight, key_weight, value_weight], axis=1),
        out_weight, inner_weight, outer_weight, packed,
    )
    qkv_g, out_g, inner_g, outer_g, vec_g, x_row, cot_row = gather_all(
        shards, layer_in, cotangent, depth, seq_size
    )
    qkv_mat = qkv_g.reshape(features, 3 * features)
    out_mat = out_g.reshape(features, features)
    inner_mat = inner_g.reshape(features, hidden_units)
    outer_mat = outer_g.reshape(hidden_units, features)
    flat = vec_g.reshape(devices, 1024).astype(f32)
    vecs = [flat[:, j * narrow : (j + 1) * narrow].reshape(features) for j in range(8)]
    query_vec, value_vec, out_vec, attn_g, attn_s, outer_vec, final_g, final_s = vecs
    inner_vec = flat[:, 8 * narrow : 8 * narrow + 4 * narrow].reshape(hidden_units)

    inputs = x_row.reshape(tokens, features)
    cot = cot_row.reshape(tokens, features)
    lengths = lax.dynamic_index_in_dim(seg_lengths, lax.axis_index("seq"), 0, keepdims=False)
    ends = jnp.cumsum(lengths)
    positions = jnp.arange(tokens, dtype=jnp.int32)
    seg_ids = jnp.sum((positions[:, None] >= ends[None, :]).astype(jnp.int32), axis=1)
    real = (positions < ends[-1]).astype(f32)

    qkv_vec = jnp.concatenate([query_vec, jnp.zeros_like(query_vec), value_vec])
    qkv = (jnp.dot(inputs, qkv_mat, preferred_element_type=f32) + qkv_vec).astype(bf16)
    context, lse = attend(qkv, seg_ids[:, None], seg_ids[None, :])
    first_sum = inputs.astype(f32) + jnp.dot(context, out_mat, preferred_element_type=f32) + out_vec
    normed_one, inv_std_one = norm_parts(first_sum)
    hidden = normed_one * attn_g + attn_s
    hidden_b = hidden.astype(bf16)
    inner_pre = jnp.dot(hidden_b, inner_mat, preferred_element_type=f32) + inner_vec
    active, slope = gelu_parts(inner_pre)
    active, slope = active.astype(bf16), slope.astype(bf16)
    outer_out = jnp.dot(active, outer_mat, preferred_element_type=f32) + outer_vec
    normed_two, inv_std_two = norm_parts(hidden + outer_out)
    layer_out = (normed_two * final_g + final_s).astype(bf16)

    upstream = cot.astype(f32) * real[:, None]
    grad_final_gain = jnp.sum(upstream * normed_two, axis=0)
    grad_final_shift = jnp.sum(upstream, axis=0)
    grad_second = norm_back(upstream, normed_two, inv_std_two, final_g)
    grad_outer = grad_second.astype(bf16)
    grad_outer_bias = jnp.sum(grad_outer.astype(f32), axis=0)
    grad_outer_weight = jnp.einsum("tf,td->fd", active, grad_outer, preferred_element_type=f32)
    grad_active = jnp.einsum("td,fd->tf", grad_outer, outer_mat, preferred_element_type=f32)
    grad_inner = (grad_active * slope.astype(f32)).astype(bf16)
    grad_inner_bias = jnp.sum(grad_inner.astype(f32), axis=0)
    grad_inner_weight = jnp.einsum("td,tf->df", hidden_b, grad_inner, preferred_element_type=f32)
    grad_hidden = grad_second + jnp.einsum("tf,df->td", grad_inner, inner_mat, preferred_element_type=f32)
    grad_attn_gain = jnp.sum(grad_hidden * normed_one, axis=0)
    grad_attn_shift = jnp.sum(grad_hidden, axis=0)
    grad_first = norm_back(grad_hidden, normed_one, inv_std_one, attn_g)
    grad_attended = grad_first.astype(bf16)
    grad_out_bias = jnp.sum(grad_attended.astype(f32), axis=0)
    grad_out_weight = jnp.einsum("td,te->de", context, grad_attended, preferred_element_type=f32)
    grad_context = jnp.einsum("te,de->td", grad_attended, out_mat, preferred_element_type=f32).astype(bf16)
    grad_qkv = attend_grad(qkv, grad_context, lse, seg_ids[:, None], seg_ids[None, :])
    grad_qkv_weight = jnp.einsum("td,te->de", inputs, grad_qkv, preferred_element_type=f32)
    grad_qkv_bias = jnp.sum(grad_qkv.astype(f32), axis=0)
    grad_in = grad_first + jnp.einsum("te,de->td", grad_qkv, qkv_mat, preferred_element_type=f32)

    narrow_grads = (
        grad_qkv_bias[:features], grad_qkv_bias[2 * features :], grad_out_bias, grad_attn_gain,
        grad_attn_shift, grad_outer_bias, grad_final_gain, grad_final_shift, grad_inner_bias,
    )
    vec_p = jnp.concatenate([v.reshape(devices, -1) for v in narrow_grads], axis=1)
    vec_p = jnp.pad(vec_p, ((0, 0), (0, 1024 - vec_p.shape[1])))
    lead = (2, 2, depth, 2)
    partials = (
        grad_qkv_weight.astype(bf16).reshape(lead + (-1, 3 * features)),
        grad_out_weight.astype(bf16).reshape(lead + (-1, features)),
        grad_inner_weight.astype(bf16).reshape(lead + (-1, hidden_units)),
        grad_outer_weight.astype(bf16).reshape(lead + (-1, features)),
        vec_p.reshape(lead + (8, 128)),
    )
    blocks = (row_count, block_len, features)
    qkv_r, out_r, inner_r, outer_r, vec_r, layer_out, grad_in = reduce_all(
        partials, layer_out.reshape(blocks), grad_in.astype(bf16).reshape(blocks), depth, seq_size
    )
    owned = vec_r.reshape(1024)
    g_qb, g_vb, g_ob, g_ag, g_as, g_tb, g_fg, g_fs = [owned[j * narrow : (j + 1) * narrow] for j in range(8)]
    g_ib = owned[8 * narrow : 12 * narrow]
    return (
        layer_out, grad_in.astype(f32),
        qkv_r[:, :features], g_qb, qkv_r[:, features : 2 * features], qkv_r[:, 2 * features :], g_vb,
        out_r, g_ob, g_ag, g_as, inner_r, g_ib, outer_r, g_tb, g_fg, g_fs,
    )


def solution(mesh):
    placed = (
        P("rows", "seq", None),
        P("rows", "seq", None),
        P("rows", None),
        P(("rows", "seq"), None),
        P(("rows", "seq")),
        P(("rows", "seq"), None),
        P(("rows", "seq"), None),
        P(("rows", "seq")),
        P(("rows", "seq"), None),
        P(("rows", "seq")),
        P(("rows", "seq")),
        P(("rows", "seq")),
        P(("rows", "seq"), None),
        P(("rows", "seq")),
        P(("rows", "seq"), None),
        P(("rows", "seq")),
        P(("rows", "seq")),
        P(("rows", "seq")),
    )
    by_row = mesh.shape["rows"] == 4 and mesh.shape["seq"] == 8
    return jax.shard_map(
        row_body if by_row else body,
        mesh=mesh,
        in_specs=placed,
        out_specs=(
            P("rows", "seq", None),
            P("rows", "seq", None),
            P(("rows", "seq"), None),
            P(("rows", "seq")),
            P(("rows", "seq"), None),
            P(("rows", "seq"), None),
            P(("rows", "seq")),
            P(("rows", "seq"), None),
            P(("rows", "seq")),
            P(("rows", "seq")),
            P(("rows", "seq")),
            P(("rows", "seq"), None),
            P(("rows", "seq")),
            P(("rows", "seq"), None),
            P(("rows", "seq")),
            P(("rows", "seq")),
            P(("rows", "seq")),
        ),
        check_vma=False,
    )
```
